64 devices in a mesh: rep: 8 (over x, y, core), dp: 8 (over z).
Axes of the slice: x: 2, y: 2, z: 8, core: 2. Of those that a mesh axis runs over, the one named last changes fastest.
The devices are a block of a 4x4x8 slice.
Arguments:
- g_w_gate: bfloat16 [64, 2, 640, 1536], P(('rep', 'dp')), parts along dimension 0
- g_w_up: bfloat16 [64, 2, 640, 1536], P(('rep', 'dp')), parts along dimension 0
- g_w_down: bfloat16 [64, 2, 1536, 640], P(('rep', 'dp')), parts along dimension 0
- w_gate: bfloat16 [2, 640, 1536], replicated
- w_up: bfloat16 [2, 640, 1536], replicated
- w_down: bfloat16 [2, 1536, 640], replicated
- m_w_gate: float32 [2, 640, 1536], P(None, 'dp')
- m_w_up: float32 [2, 640, 1536], P(None, 'dp')
- m_w_down: float32 [2, 1536, 640], P(None, 'dp')
- v_w_gate: float32 [2, 640, 1536], P(None, 'dp')
- v_w_up: float32 [2, 640, 1536], P(None, 'dp')
- v_w_down: float32 [2, 1536, 640], P(None, 'dp')
Outputs:
- output 1: bfloat16 [16, 640, 1536], P('rep'), parts along dimension 0
- output 2: bfloat16 [16, 640, 1536], P('rep'), parts along dimension 0
- output 3: bfloat16 [16, 1536, 640], P('rep'), parts along dimension 0
- output 4: float32 [16, 640, 1536], P('rep', 'dp'), parts along dimension 0
- output 5: float32 [16, 640, 1536], P('rep', 'dp'), parts along dimension 0
- output 6: float32 [16, 1536, 640], P('rep', 'dp'), parts along dimension 0
- output 7: float32 [16, 640, 1536], P('rep', 'dp'), parts along dimension 0
- output 8: float32 [16, 640, 1536], P('rep', 'dp'), parts along dimension 0
- output 9: float32 [16, 1536, 640], P('rep', 'dp'), parts along dimension 0
There are 8 independent parts. The reference program is written for one: setup_inputs(seed, part) draws one part's arguments, and reference() takes and returns one part's arrays. A program takes and returns all parts, laid end to end along the dimension named above; an argument that names none is the same for every part.
All inputs are finite; a program needn't handle non-finite values.
Results may differ from the reference program's by a relative error of at most 0.022.
Values are sent between devices in bfloat16 or wider.
A program may use at most 768 MiB of HBM per device.

```python
import jax
import jax.numpy as jnp
from jax import lax

DEVICES = 8
D = 640
FF = 1536
LAYERS = 2
NAMES = ("w_gate", "w_up", "w_down")
SHAPES = {"w_gate": (LAYERS, D, FF), "w_up": (LAYERS, D, FF), "w_down": (LAYERS, FF, D)}


def setup_inputs(seed: int = 0, part: int = 0) -> dict:
    kz, *keys = jax.random.split(jax.random.key(seed), 1 + 5 * len(NAMES))
    loud = 2.0 ** jax.random.uniform(kz, (), jnp.float32, -1.0, 1.0)
    drawn = {}
    for name, key, both in zip(NAMES, keys[:3], keys[3:6], strict=True):
        own = jax.random.normal(jax.random.fold_in(key, part), (DEVICES, *SHAPES[name]), jnp.float32)
        shared = jax.random.normal(jax.random.fold_in(both, part), SHAPES[name], jnp.float32)
        drawn["g_" + name] = (loud * (0.7 * shared / DEVICES + 0.7 * own * DEVICES**-0.5)).astype(jnp.bfloat16)
    for name, key in zip(NAMES, keys[6:9], strict=True):
        drawn[name] = (jax.random.normal(key, SHAPES[name], jnp.float32) * SHAPES[name][1] ** -0.5).astype(jnp.bfloat16)
    for name, key in zip(NAMES, keys[9:12], strict=True):
        drawn["m_" + name] = loud * 0.5 * jax.random.normal(key, SHAPES[name], jnp.float32)
    for name, key in zip(NAMES, keys[12:15], strict=True):
        drawn["v_" + name] = loud * loud * jax.random.uniform(key, SHAPES[name], jnp.float32, 0.5, 1.5)
    return drawn


def adamw(w, m, v, g):
    m = 0.9 * m + 0.1 * g
    v = 0.95 * v + 0.05 * g * g
    step = m * lax.rsqrt(v + 1e-8) + 0.1 * w
    return (w - 0.02 * step).astype(jnp.bfloat16), m, v


def clipped(gradients, sum_of_squares, count):
    factor = jnp.minimum(1.0, 0.5 * lax.rsqrt(sum_of_squares / count + 1e-30))
    return [g * factor for g in gradients]


def reference(g_w_gate, g_w_up, g_w_down, w_gate, w_up, w_down, m_w_gate, m_w_up, m_w_down, v_w_gate, v_w_up, v_w_down):
    def total(terms):
        return lax.scan(lambda so_far, term: (so_far + term.astype(jnp.float32), None), jnp.zeros(terms.shape[1:], jnp.float32), terms)[0]

    gradients = [total(terms).astype(jnp.bfloat16).astype(jnp.float32) for terms in (g_w_gate, g_w_up, g_w_down)]
    gradients = clipped(gradients, sum(jnp.sum(g * g) for g in gradients), sum(g.size for g in gradients))
    new = [
        adamw(w.astype(jnp.float32), m, v, g)
        for w, m, v, g in zip((w_gate, w_up, w_down), (m_w_gate, m_w_up, m_w_down), (v_w_gate, v_w_up, v_w_down), gradients, strict=True)
    ]
    return tuple(one[which] for which in range(3) for one in new)
```

```python
import functools

import jax
import jax.numpy as jnp
from jax import lax
from jax.experimental import pallas as pl
from jax.experimental.pallas import tpu as pltpu
from jax.sharding import PartitionSpec as P

WAYS = (1, -1)


def row_blocks(rows, columns):
    best = 16
    for step in range(16, rows + 1, 16):
        if rows % step == 0 and step * columns <= 32 * 1024:
            best = step
    return best


def kernel(n, layers, count, *refs):
    kinds = 3
    g, w, m, v = (refs[i : i + kinds] for i in range(0, 4 * kinds, kinds))
    refs = refs[4 * kinds :]
    new_w, new_m, new_v = (refs[i : i + kinds] for i in range(0, 3 * kinds, kinds))
    refs = refs[3 * kinds :]
    own, term, got = (refs[i : i + kinds] for i in range(0, 3 * kinds, kinds))
    squares, rs_send, rs_recv, ag_send, ag_recv, sq_send, sq_recv, load_own, load_term, load_state = refs[3 * kinds :]
    half = n // 2
    me = lax.axis_index("dp")
    rows = [ref.shape[1] for ref in own]
    across = [lax.rem(me + way + n, n) for way in WAYS]
    pairs = [(layer, kind) for layer in range(layers) for kind in range(kinds)]

    def at(way, steps):
        return lax.rem(me + WAYS[way] * steps + n, n)

    def block(chunk, kind):
        return pl.ds(pl.multiple_of(chunk * rows[kind], 16), rows[kind])

    def remote(src, dst, send, recv, to):
        copy = pltpu.make_async_remote_copy(src, dst, send, recv, device_id={"dp": to}, device_id_type=pl.DeviceIdType.MESH)
        return copy

    barrier = pltpu.get_barrier_semaphore()
    for to in across:
        pl.semaphore_signal(barrier, inc=1, device_id={"dp": to}, device_id_type=pl.DeviceIdType.MESH)
    pl.semaphore_wait(barrier, len(WAYS))

    def halved(way):
        return range(way * layers // 2, (way + 1) * layers // 2)

    def slot(step, layer, way):
        return layer - halved(way)[0] if step == 1 else layers // 2 + (step - 2) * layers + layer

    def term_slot(step, layer, way):
        return layer - halved(way)[0] if step == 2 else layers // 2 + (step - 3) * layers + layer

    sums = {}

    def send_sum(way, step, layer, kind, src):
        here = slot(step, layer, way)
        sems = (rs_send.at[way, here, kind], rs_recv.at[way, here, kind])
        sums[way, step, layer, kind] = remote(src, got[kind].at[way, here], *sems, across[way])
        sums[way, step, layer, kind].start()

    for kind in range(kinds):
        for i in range(layers // 2):
            for way in range(2):
                layer = halved(way)[i]
                send_sum(way, 1, layer, kind, g[kind].at[layer, block(at(way, half), kind)])
    for kind in range(kinds):
        for i in range(layers // 2):
            for way in range(2):
                layer = halved(1 - way)[i]
                send_sum(way, 2, layer, kind, g[kind].at[layer, block(at(way, half - 1), kind)])

    loads = {}
    for step in range(2, half + 1):
        for way in range(2):
            first = halved(way)[0] if step == 2 else 0
            many = layers // 2 if step == 2 else layers
            for kind in range(kinds):
                src = g[kind].at[pl.ds(first, many), block(at(way, half + 1 - step), kind)]
                dst = term[kind].at[way, pl.ds(term_slot(step, first, way), many)]
                loads[way, step, kind] = pltpu.make_async_copy(src, dst, load_term.at[way, step - 2, kind])
                loads[way, step, kind].start()
    for kind in range(kinds):
        loads[kind] = pltpu.make_async_copy(g[kind].at[:, block(me, kind)], own[kind], load_own.at[kind])
        loads[kind].start()
    states = []
    for kind in range(kinds):
        here = block(me, kind)
        for which, (src, dst) in enumerate(
            ((m[kind], new_m[kind]), (v[kind], new_v[kind]), (w[kind].at[:, here], new_w[kind].at[:, here]))
        ):
            states.append(pltpu.make_async_copy(src, dst, load_state.at[which, kind]))
            states[-1].start()

    def each_rows(kind, body, carry=None):
        many = row_blocks(rows[kind], own[kind].shape[2])

        def one(i, carry):
            return body(pl.ds(pl.multiple_of(i * many, many), many), carry)

        return lax.fori_loop(0, rows[kind] // many, one, carry)

    def pass_on(way, step, layer, kind):
        sums[way, step - 1, layer, kind].wait_recv()
        into = got[kind].at[way, slot(step - 1, layer, way)]
        mine = term[kind].at[way, term_slot(step, layer, way)]

        def add(r, _):
            into[r] = (into[r].astype(jnp.float32) + mine[r].astype(jnp.float32)).astype(jnp.bfloat16)

        each_rows(kind, add)
        send_sum(way, step, layer, kind, into)

    waited = set()

    def loaded(*key):
        if key not in waited:
            waited.add(key)
            loads[key if len(key) > 1 else key[0]].wait()

    for kind in range(kinds):
        for i in range(layers // 2):
            for way in range(2):
                loaded(way, 2, kind)
                pass_on(way, 2, halved(way)[i], kind)
    for step in range(3, half + 1):
        for j in range(layers):
            for kind in range(kinds):
                for way in range(2):
                    order = (*halved(1 - way), *halved(way)) if step < half else range(layers)
                    loaded(way, step, kind)
                    pass_on(way, step, order[j], kind)

    total = jnp.zeros((8, 128), jnp.float32)
    for layer, kind in pairs:
        loaded(kind)
        for way in range(2):
            sums[way, half, layer, kind].wait_recv()
        ends = [got[kind].at[way, slot(half, layer, way)] for way in range(2)]
        mine = own[kind].at[layer]

        def finish(r, total):
            x = mine[r].astype(jnp.float32) + ends[0][r].astype(jnp.float32) + ends[1][r].astype(jnp.float32)
            x = x.astype(jnp.bfloat16)
            mine[r] = x
            x = x.astype(jnp.float32)
            x = x * x
            parts = [x[i : i + 8, j : j + 128] for i in range(0, x.shape[0], 8) for j in range(0, x.shape[1], 128)]
            while len(parts) > 1:
                parts = [a + b for a, b in zip(parts[::2], parts[1::2])] + ([parts[-1]] if len(parts) % 2 else [])
            return total + parts[0]

        total = each_rows(kind, finish, total)

    squares[me] = total
    told = []
    for off in range(1, n):
        sems = (sq_send.at[off - 1], sq_recv.at[off - 1])
        told.append(remote(squares.at[me], squares.at[me], *sems, lax.rem(me + off, n)))
        told[-1].start()
    for copy in states:
        copy.wait()
    for copy in told:
        copy.wait_recv()
    total = jnp.sum(squares[...], axis=0)
    total = jnp.sum(jnp.sum(total, axis=1, keepdims=True), axis=0, keepdims=True)
    factor = jnp.minimum(1.0, 0.5 * lax.rsqrt(total / count + 1e-30))

    gathers = {}

    def send_new(way, step, layer, kind):
        here = new_w[kind].at[layer, block(at(way, 1 - step), kind)]
        sems = (ag_send.at[way, step - 1, layer, kind], ag_recv.at[way, step - 1, layer, kind])
        gathers[way, step, layer, kind] = remote(here, here, *sems, across[way])
        gathers[way, step, layer, kind].start()

    for layer, kind in pairs:
        grad, m_at, v_at = own[kind].at[layer], new_m[kind].at[layer], new_v[kind].at[layer]
        base = pl.multiple_of(me * rows[kind], 16)
        w_at = new_w[kind].at[layer]

        def adamw(r, _):
            x = grad[r].astype(jnp.float32) * factor
            there = pl.ds(pl.multiple_of(base + r.start, 16), r.size)
            old = w_at[there].astype(jnp.float32)
            m_new = 0.9 * m_at[r] + 0.1 * x
            v_new = 0.95 * v_at[r] + 0.05 * x * x
            m_at[r] = m_new
            v_at[r] = v_new
            step = m_new * lax.rsqrt(v_new + 1e-8) + 0.1 * old
            w_at[there] = (old - 0.02 * step).astype(jnp.bfloat16)

        each_rows(kind, adamw)
        for way in range(2):
            send_new(way, 1, layer, kind)
    for step in range(1, half + 1):
        for layer, kind in pairs:
            for way in range(2):
                if step < half or layer in halved(way):
                    gathers[way, step, layer, kind].wait_recv()
                    if step < half - 1 or (step == half - 1 and layer in halved(way)):
                        send_new(way, step + 1, layer, kind)
    for copy in (*sums.values(), *told, *gathers.values()):
        copy.wait_send()


def solution(mesh):
    n = mesh.shape["dp"]

    def step(*arrays):
        terms, weights, m, v = (arrays[i : i + 3] for i in (0, 3, 6, 9))
        terms = [t[0] for t in terms]
        layers = m[0].shape[0]
        shapes = [one.shape[1:] for one in m]
        count = n * sum(one.size for one in m)
        half = n // 2
        sums = layers // 2 + (half - 1) * layers
        terms_kept = layers // 2 + (half - 2) * layers
        dma = pltpu.SemaphoreType.DMA
        scratch = [pltpu.VMEM((layers, *s), jnp.bfloat16) for s in shapes]
        scratch += [pltpu.VMEM((2, terms_kept, *s), jnp.bfloat16) for s in shapes]
        scratch += [pltpu.VMEM((2, sums, *s), jnp.bfloat16) for s in shapes]
        scratch += [pltpu.VMEM((n, 8, 128), jnp.float32)]
        scratch += [dma((2, sums, 3)), dma((2, sums, 3)), dma((2, half, layers, 3)), dma((2, half, layers, 3))]
        scratch += [dma((n - 1,)), dma((n - 1,)), dma((3,)), dma((2, half - 1, 3)), dma((3, 3))]
        out = [pltpu.VMEM(one.shape, one.dtype) for one in (*weights, *m, *v)]
        return pl.pallas_call(
            functools.partial(kernel, n, layers, count),
            out_shape=out,
            in_specs=[pl.BlockSpec(memory_space=pltpu.HBM)] * 12,
            out_specs=[pl.BlockSpec(memory_space=pltpu.VMEM)] * 9,
            scratch_shapes=scratch,
            compiler_params=pltpu.CompilerParams(collective_id=0, has_side_effects=True, vmem_limit_bytes=40 * 2**20),
        )(*terms, *weights, *m, *v)

    all_of, cut = P(None, None, None), P(None, "dp", None)
    return jax.shard_map(
        step,
        mesh=mesh,
        in_specs=(P(("rep", "dp"), None, None, None),) * 3 + (all_of,) * 3 + (cut,) * 6,
        out_specs=(P("rep", None, None),) * 3 + (P("rep", "dp", None),) * 6,
        check_vma=False,
    )
```

```python
import functools

import jax
import jax.numpy as jnp
from jax import lax
from jax.experimental import pallas as pl
from jax.experimental.pallas import tpu as pltpu
from jax.sharding import PartitionSpec as P

WAYS = (1, -1)


def row_blocks(rows, columns):
    best = 16
    for step in range(16, rows + 1, 16):
        if rows % step == 0 and step * columns <= 32 * 1024:
            best = step
    return best


def kernel(n, layers, count, *refs):
    kinds = 3
    g, w, m, v = (refs[i : i + kinds] for i in range(0, 4 * kinds, kinds))
    refs = refs[4 * kinds :]
    new_w, new_m, new_v = (refs[i : i + kinds] for i in range(0, 3 * kinds, kinds))
    refs = refs[3 * kinds :]
    own, term, got = (refs[i : i + kinds] for i in range(0, 3 * kinds, kinds))
    squares, arrived, rs_send, ag_send, sq_send, sq_recv, load_own, load_term, load_state = refs[3 * kinds :]
    half = n // 2
    me = lax.axis_index("dp")
    rows = [ref.shape[1] for ref in own]
    across = [lax.rem(me + way + n, n) for way in WAYS]
    pairs = [(layer, kind) for layer in range(layers) for kind in range(kinds)]

    def at(way, steps):
        return lax.rem(me + WAYS[way] * steps + n, n)

    def block(chunk, kind):
        return pl.ds(pl.multiple_of(chunk * rows[kind], 16), rows[kind])

    def remote(src, dst, send, recv, to):
        copy = pltpu.make_async_remote_copy(src, dst, send, recv, device_id={"dp": to}, device_id_type=pl.DeviceIdType.MESH)
        return copy

    barrier = pltpu.get_barrier_semaphore()
    for to in across:
        pl.semaphore_signal(barrier, inc=1, device_id={"dp": to}, device_id_type=pl.DeviceIdType.MESH)
    pl.semaphore_wait(barrier, len(WAYS))

    def halved(way):
        return range(way * layers // 2, (way + 1) * layers // 2)

    def slot(step, layer, way):
        return layer - halved(way)[0] if step == 1 else layers // 2 + (step - 2) * layers + layer

    def term_slot(step, layer, way):
        return layer - halved(way)[0] if step == 2 else layers // 2 + (step - 3) * layers + layer

    sums = {}

    def send_sum(way, step, layer, kind, src):
        here = slot(step, layer, way)
        sems = (rs_send.at[kind], arrived.at[way, here, kind])
        sums[way, step, layer, kind] = remote(src, got[kind].at[way, here], *sems, across[way])
        sums[way, step, layer, kind].start()

    def fetch():
        for kind in range(kinds):
            for step in range(2, half + 1):
                for way in range(2):
                    first = halved(way)[0] if step == 2 else 0
                    many = layers // 2 if step == 2 else layers
                    src = g[kind].at[pl.ds(first, many), block(at(way, half + 1 - step), kind)]
                    dst = term[kind].at[way, pl.ds(term_slot(step, first, way), many)]
                    pltpu.make_async_copy(src, dst, load_term.at[kind]).start()
        copies = []
        for kind in range(kinds):
            here = block(me, kind)
            copies.append(pltpu.make_async_copy(g[kind].at[:, here], own[kind], load_own.at[kind]))
            copies.append(pltpu.make_async_copy(m[kind], new_m[kind], load_state.at[0, kind]))
            copies.append(pltpu.make_async_copy(v[kind], new_v[kind], load_state.at[1, kind]))
            copies.append(pltpu.make_async_copy(w[kind].at[:, here], new_w[kind].at[:, here], load_state.at[2, kind]))
        for copy in copies:
            copy.start()
        for kind in range(kinds):
            pltpu.make_async_copy(term[kind], term[kind], load_term.at[kind]).wait()
        for copy in copies:
            copy.wait()

    late = lax.rem(lax.axis_index("rep"), 2) == 0

    @pl.when(late)
    def _():
        fetch()

    for kind in range(kinds):
        for i in range(layers // 2):
            for way in range(2):
                layer = halved(way)[i]
                send_sum(way, 1, layer, kind, g[kind].at[layer, block(at(way, half), kind)])
    for kind in range(kinds):
        for i in range(layers // 2):
            for way in range(2):
                layer = halved(1 - way)[i]
                send_sum(way, 2, layer, kind, g[kind].at[layer, block(at(way, half - 1), kind)])

    @pl.when(jnp.logical_not(late))
    def _():
        fetch()

    def each_rows(kind, body, carry=None):
        many = row_blocks(rows[kind], own[kind].shape[2])

        def one(i, carry):
            return body(pl.ds(pl.multiple_of(i * many, many), many), carry)

        return lax.fori_loop(0, rows[kind] // many, one, carry)

    def pass_on(way, step, layer, kind):
        sums[way, step - 1, layer, kind].wait_recv()
        into = got[kind].at[way, slot(step - 1, layer, way)]
        mine = term[kind].at[way, term_slot(step, layer, way)]

        def add(r, _):
            into[r] = (into[r].astype(jnp.float32) + mine[r].astype(jnp.float32)).astype(jnp.bfloat16)

        each_rows(kind, add)
        send_sum(way, step, layer, kind, into)

    for kind in range(kinds):
        for i in range(layers // 2):
            for way in range(2):
                pass_on(way, 2, halved(way)[i], kind)
    for step in range(3, half + 1):
        for j in range(layers):
            for kind in range(kinds):
                for way in range(2):
                    order = (*halved(1 - way), *halved(way)) if step < half else range(layers)
                    pass_on(way, step, order[j], kind)

    total = jnp.zeros((8, 128), jnp.float32)
    for layer, kind in pairs:
        for way in range(2):
            sums[way, half, layer, kind].wait_recv()
        ends = [got[kind].at[way, slot(half, layer, way)] for way in range(2)]
        mine = own[kind].at[layer]

        def finish(r, total):
            x = mine[r].astype(jnp.float32) + ends[0][r].astype(jnp.float32) + ends[1][r].astype(jnp.float32)
            x = x.astype(jnp.bfloat16)
            mine[r] = x
            x = x.astype(jnp.float32)
            x = x * x
            parts = [x[i : i + 8, j : j + 128] for i in range(0, x.shape[0], 8) for j in range(0, x.shape[1], 128)]
            while len(parts) > 1:
                parts = [a + b for a, b in zip(parts[::2], parts[1::2])] + ([parts[-1]] if len(parts) % 2 else [])
            return total + parts[0]

        total = each_rows(kind, finish, total)

    squares[me] = total
    told = []
    for off in range(1, n):
        told.append(remote(squares.at[me], squares.at[me], sq_send.at[0], sq_recv.at[0], lax.rem(me + off, n)))
        told[-1].start()
    others = squares.at[pl.ds(0, n - 1)]
    pltpu.make_async_copy(others, others, sq_recv.at[0]).wait()
    total = jnp.sum(squares[...], axis=0)
    total = jnp.sum(jnp.sum(total, axis=1, keepdims=True), axis=0, keepdims=True)
    factor = jnp.minimum(1.0, 0.5 * lax.rsqrt(total / count + 1e-30))

    gathers = {}

    def gather_slot(way, step, layer):
        return (step - 1) * layers + (layer if step < half else layer - halved(way)[0])

    def send_new(way, step, layer, kind):
        here = new_w[kind].at[layer, block(at(way, 1 - step), kind)]
        sems = (ag_send.at[kind], arrived.at[way, gather_slot(way, step, layer), kind])
        gathers[way, step, layer, kind] = remote(here, here, *sems, across[way])
        gathers[way, step, layer, kind].start()

    for layer, kind in pairs:
        grad, m_at, v_at = own[kind].at[layer], new_m[kind].at[layer], new_v[kind].at[layer]
        base = pl.multiple_of(me * rows[kind], 16)
        w_at = new_w[kind].at[layer]

        def adamw(r, _):
            x = grad[r].astype(jnp.float32) * factor
            there = pl.ds(pl.multiple_of(base + r.start, 16), r.size)
            old = w_at[there].astype(jnp.float32)
            m_new = 0.9 * m_at[r] + 0.1 * x
            v_new = 0.95 * v_at[r] + 0.05 * x * x
            m_at[r] = m_new
            v_at[r] = v_new
            step = m_new * lax.rsqrt(v_new + 1e-8) + 0.1 * old
            w_at[there] = (old - 0.02 * step).astype(jnp.bfloat16)

        each_rows(kind, adamw)
        for way in range(2):
            send_new(way, 1, layer, kind)
    for step in range(1, half + 1):
        for layer, kind in pairs:
            for way in range(2):
                if step < half or layer in halved(way):
                    gathers[way, step, layer, kind].wait_recv()
                    if step < half - 1 or (step == half - 1 and layer in halved(way)):
                        send_new(way, step + 1, layer, kind)
    for kind in range(kinds):
        for sem in (rs_send, ag_send):
            pltpu.make_async_copy(got[kind], got[kind], sem.at[kind]).wait()
    pltpu.make_async_copy(others, others, sq_send.at[0]).wait()


def write_out(*refs):
    n = (len(refs) - 1) // 2
    copies = [pltpu.make_async_copy(src, dst, refs[-1].at[i]) for i, (src, dst) in enumerate(zip(refs[:n], refs[n : 2 * n]))]
    for copy in copies:
        copy.start()
    for copy in copies:
        copy.wait()


def solution(mesh):
    n = mesh.shape["dp"]

    def step(*arrays):
        terms, weights, m, v = (arrays[i : i + 3] for i in (0, 3, 6, 9))
        terms = [t[0] for t in terms]
        layers = m[0].shape[0]
        shapes = [one.shape[1:] for one in m]
        count = n * sum(one.size for one in m)
        half = n // 2
        sums = layers // 2 + (half - 1) * layers
        terms_kept = layers // 2 + (half - 2) * layers
        dma = pltpu.SemaphoreType.DMA
        scratch = [pltpu.VMEM((layers, *s), jnp.bfloat16) for s in shapes]
        scratch += [pltpu.VMEM((2, terms_kept, *s), jnp.bfloat16) for s in shapes]
        scratch += [pltpu.VMEM((2, sums, *s), jnp.bfloat16) for s in shapes]
        scratch += [pltpu.VMEM((n, 8, 128), jnp.float32)]
        scratch += [dma((2, sums, 3)), dma((3,)), dma((3,)), dma((1,)), dma((1,)), dma((3,)), dma((3,)), dma((3, 3))]
        out = [pltpu.VMEM(one.shape, one.dtype) for one in (*weights, *m, *v)]
        kept = pl.pallas_call(
            functools.partial(kernel, n, layers, count),
            out_shape=out,
            in_specs=[pl.BlockSpec(memory_space=pltpu.HBM)] * 12,
            out_specs=[pl.BlockSpec(memory_space=pltpu.VMEM)] * 9,
            scratch_shapes=scratch,
            compiler_params=pltpu.CompilerParams(collective_id=0, has_side_effects=True, vmem_limit_bytes=40 * 2**20),
        )(*terms, *weights, *m, *v)
        return pl.pallas_call(
            write_out,
            out_shape=[jax.ShapeDtypeStruct(one.shape, one.dtype) for one in kept],
            in_specs=[pl.BlockSpec(memory_space=pltpu.VMEM)] * 9,
            out_specs=[pl.BlockSpec(memory_space=pltpu.HBM)] * 9,
            scratch_shapes=[dma((9,))],
            compiler_params=pltpu.CompilerParams(vmem_limit_bytes=2**20),
        )(*kept)

    all_of, cut = P(None, None, None), P(None, "dp", None)
    return jax.shard_map(
        step,
        mesh=mesh,
        in_specs=(P(("rep", "dp"), None, None, None),) * 3 + (all_of,) * 3 + (cut,) * 6,
        out_specs=(P("rep", None, None),) * 3 + (P("rep", "dp", None),) * 6,
        check_vma=False,
    )
```

```python
import functools

import jax
import jax.numpy as jnp
from jax import lax
from jax.experimental import pallas as pl
from jax.experimental.pallas import tpu as pltpu
from jax.sharding import PartitionSpec as P

WAYS = (1, -1)
LAG_NS = 5000


def row_blocks(rows, columns):
    best = 16
    for step in range(16, rows + 1, 16):
        if rows % step == 0 and step * columns <= 32 * 1024:
            best = step
    return best


def remote(src, dst, send, recv, to):
    return pltpu.make_async_remote_copy(src, dst, send, recv, device_id={"dp": to}, device_id_type=pl.DeviceIdType.MESH)


def meet(n):
    me = lax.axis_index("dp")

    def at(way, steps):
        return lax.rem(me + WAYS[way] * steps + n, n)

    barrier = pltpu.get_barrier_semaphore()
    for way in range(2):
        pl.semaphore_signal(barrier, inc=1, device_id={"dp": at(way, 1)}, device_id_type=pl.DeviceIdType.MESH)
    pl.semaphore_wait(barrier, 2)
    return me, at


def halved(layers, way):
    return range(way * layers // 2, (way + 1) * layers // 2)


class Gather:
    def __init__(self, n, at, outs, rows, arrived, sent):
        self.half, self.at, self.outs, self.rows, self.arrived, self.sent = n // 2, at, outs, rows, arrived, sent
        self.n, self.layers, self.copies = n, outs[0].shape[0], {}

    def block(self, chunk, kind):
        return pl.ds(pl.multiple_of(chunk * self.rows[kind], 16), self.rows[kind])

    def send(self, way, step, layer, kind, src=None):
        here = self.outs[kind].at[layer, self.block(self.at(way, 1 - step), kind)]
        slot = (step - 1) * self.layers + (layer if step < self.half else layer - halved(self.layers, way)[0])
        copy = remote(here if src is None else src, here, self.sent.at[kind], self.arrived.at[way, slot, kind], self.at(way, 1))
        self.copies[way, step, layer, kind] = copy
        copy.start()

    def run(self):
        for step in range(1, self.half + 1):
            for i in range(self.layers):
                for kind in range(len(self.outs)):
                    for way in range(2):
                        far = halved(self.layers, way)
                        layer = (*far, *halved(self.layers, 1 - way))[i]
                        if step == self.half and layer not in far:
                            continue
                        self.copies[way, step, layer, kind].wait_recv()
                        if step < self.half - 1 or (step == self.half - 1 and layer in far):
                            self.send(way, step + 1, layer, kind)
        for kind, out in enumerate(self.outs):
            moved = out.at[:, pl.ds(0, (self.n - 1) * self.rows[kind])]
            pltpu.make_async_copy(moved, moved, self.sent.at[kind]).wait()


def sum_and_step(n, layers, count, *refs):
    kinds = 3
    g, w, m, v = (refs[i : i + kinds] for i in range(0, 4 * kinds, kinds))
    refs = refs[4 * kinds :]
    new_w, new_m, new_v = (refs[i : i + kinds] for i in range(0, 3 * kinds, kinds))
    refs = refs[3 * kinds :]
    own, term, got = (refs[i : i + kinds] for i in range(0, 3 * kinds, kinds))
    squares, arrived, rs_send, ag_send, sq_send, sq_recv, load_own, load_term, load_state = refs[3 * kinds :]
    half = n // 2
    rows = [ref.shape[1] for ref in own]
    pairs = [(layer, kind) for kind in range(kinds) for layer in range(layers)]
    me, at = meet(n)

    def block(chunk, kind):
        return pl.ds(pl.multiple_of(chunk * rows[kind], 16), rows[kind])

    def slot(step, layer, way):
        return layer - halved(layers, way)[0] if step == 1 else layers // 2 + (step - 2) * layers + layer

    def term_slot(step, layer, way):
        return layer - halved(layers, way)[0] if step == 2 else layers // 2 + (step - 3) * layers + layer

    sums = {}

    def send_sum(way, step, layer, kind, src):
        here = slot(step, layer, way)
        sems = (rs_send.at[kind], arrived.at[way, here, kind])
        sums[way, step, layer, kind] = remote(src, got[kind].at[way, here], *sems, at(way, 1))
        sums[way, step, layer, kind].start()

    def fetch():
        for kind in range(kinds):
            for step in range(2, half + 1):
                for way in range(2):
                    first = halved(layers, way)[0] if step == 2 else 0
                    many = layers // 2 if step == 2 else layers
                    src = g[kind].at[pl.ds(first, many), block(at(way, half + 1 - step), kind)]
                    dst = term[kind].at[way, pl.ds(term_slot(step, first, way), many)]
                    pltpu.make_async_copy(src, dst, load_term.at[kind]).start()
        copies = []
        for kind in range(kinds):
            here = block(me, kind)
            copies.append(pltpu.make_async_copy(g[kind].at[:, here], own[kind], load_own.at[kind]))
            copies.append(pltpu.make_async_copy(m[kind], new_m[kind], load_state.at[0, kind]))
            copies.append(pltpu.make_async_copy(v[kind], new_v[kind], load_state.at[1, kind]))
            to = new_w[kind].at[:, here] if kind < kinds - 1 else new_w[kind]
            copies.append(pltpu.make_async_copy(w[kind].at[:, here], to, load_state.at[2, kind]))
        for copy in copies:
            copy.start()
        for kind in range(kinds):
            pltpu.make_async_copy(term[kind], term[kind], load_term.at[kind]).wait()
        for copy in copies:
            copy.wait()

    late = lax.rem(lax.axis_index("rep"), 2) == 0

    @pl.when(late)
    def _():
        fetch()
        pl.delay(LAG_NS)

    for kind in range(kinds):
        for i in range(layers // 2):
            for way in range(2):
                layer = halved(layers, way)[i]
                send_sum(way, 1, layer, kind, g[kind].at[layer, block(at(way, half), kind)])
    for kind in range(kinds):
        for i in range(layers // 2):
            for way in range(2):
                layer = halved(layers, 1 - way)[i]
                send_sum(way, 2, layer, kind, g[kind].at[layer, block(at(way, half - 1), kind)])

    @pl.when(jnp.logical_not(late))
    def _():
        fetch()

    def each_rows(kind, body, carry=None):
        many = row_blocks(rows[kind], own[kind].shape[2])

        def one(i, carry):
            return body(pl.ds(pl.multiple_of(i * many, many), many), carry)

        return lax.fori_loop(0, rows[kind] // many, one, carry)

    def pass_on(way, step, layer, kind):
        sums[way, step - 1, layer, kind].wait_recv()
        into = got[kind].at[way, slot(step - 1, layer, way)]
        mine = term[kind].at[way, term_slot(step, layer, way)]

        def add(r, _):
            into[r] = (into[r].astype(jnp.float32) + mine[r].astype(jnp.float32)).astype(jnp.bfloat16)

        each_rows(kind, add)
        send_sum(way, step, layer, kind, into)

    for kind in range(kinds):
        for i in range(layers // 2):
            for way in range(2):
                pass_on(way, 2, halved(layers, way)[i], kind)
    for step in range(3, half + 1):
        for j in range(layers):
            for kind in range(kinds):
                for way in range(2):
                    order = (*halved(layers, 1 - way), *halved(layers, way)) if step < half else range(layers)
                    pass_on(way, step, order[j], kind)

    total = jnp.zeros((8, 128), jnp.float32)
    for layer, kind in pairs:
        for way in range(2):
            sums[way, half, layer, kind].wait_recv()
        ends = [got[kind].at[way, slot(half, layer, way)] for way in range(2)]
        mine = own[kind].at[layer]

        def finish(r, total):
            x = mine[r].astype(jnp.float32) + ends[0][r].astype(jnp.float32) + ends[1][r].astype(jnp.float32)
            x = x.astype(jnp.bfloat16)
            mine[r] = x
            x = x.astype(jnp.float32)
            x = x * x
            parts = [x[i : i + 8, j : j + 128] for i in range(0, x.shape[0], 8) for j in range(0, x.shape[1], 128)]
            while len(parts) > 1:
                parts = [a + b for a, b in zip(parts[::2], parts[1::2])] + ([parts[-1]] if len(parts) % 2 else [])
            return total + parts[0]

        total = each_rows(kind, finish, total)

    squares[me] = total
    told = []
    for off in range(1, n):
        told.append(remote(squares.at[me], squares.at[me], sq_send.at[0], sq_recv.at[0], lax.rem(me + off, n)))
        told[-1].start()
    others = squares.at[pl.ds(0, n - 1)]
    pltpu.make_async_copy(others, others, sq_recv.at[0]).wait()
    total = jnp.sum(squares[...], axis=0)
    total = jnp.sum(jnp.sum(total, axis=1, keepdims=True), axis=0, keepdims=True)
    factor = jnp.minimum(1.0, 0.5 * lax.rsqrt(total / count + 1e-30))

    gather = Gather(n, at, new_w[: kinds - 1], rows, arrived, ag_send)
    for kind in range(kinds):
        for layer in range(layers):
            grad, m_at, v_at = own[kind].at[layer], new_m[kind].at[layer], new_v[kind].at[layer]
            base = pl.multiple_of(me * rows[kind], 16) if kind < kinds - 1 else 0
            w_at = new_w[kind].at[layer]

            def adamw(r, _):
                x = grad[r].astype(jnp.float32) * factor
                there = pl.ds(pl.multiple_of(base + r.start, 16), r.size)
                old = w_at[there].astype(jnp.float32)
                m_new = 0.9 * m_at[r] + 0.1 * x
                v_new = 0.95 * v_at[r] + 0.05 * x * x
                m_at[r] = m_new
                v_at[r] = v_new
                step = m_new * lax.rsqrt(v_new + 1e-8) + 0.1 * old
                w_at[there] = (old - 0.02 * step).astype(jnp.bfloat16)

            each_rows(kind, adamw)
            if kind < kinds - 1:
                for way in range(2):
                    gather.send(way, 1, layer, kind)
    gather.run()
    for kind in range(kinds):
        pltpu.make_async_copy(got[kind], got[kind], rs_send.at[kind]).wait()
    pltpu.make_async_copy(others, others, sq_send.at[0]).wait()


def gather_last(n, own, after, out, arrived, sent):
    me, at = meet(n)
    gather = Gather(n, at, [out], [own.shape[1]], arrived, sent)
    for i in range(own.shape[0]):
        for way in range(2):
            layer = (*halved(own.shape[0], way), *halved(own.shape[0], 1 - way))[i]
            gather.send(way, 1, layer, 0, own.at[layer])
    out[:, gather.block(me, 0)] = own[...]
    gather.run()


def write_out(*refs):
    n = (len(refs) - 2) // 2
    copies = [pltpu.make_async_copy(src, dst, refs[-1].at[i]) for i, (src, dst) in enumerate(zip(refs[:n], refs[n : 2 * n]))]
    refs[-2][...] = jnp.zeros_like(refs[-2])
    for copy in copies:
        copy.start()
    for copy in copies:
        copy.wait()


def solution(mesh):
    n = mesh.shape["dp"]

    def step(*arrays):
        terms, weights, m, v = (arrays[i : i + 3] for i in (0, 3, 6, 9))
        terms = [t[0] for t in terms]
        layers = m[0].shape[0]
        shapes = [one.shape[1:] for one in m]
        count = n * sum(one.size for one in m)
        half = n // 2
        sums = layers // 2 + (half - 1) * layers
        terms_kept = layers // 2 + (half - 2) * layers
        dma = pltpu.SemaphoreType.DMA
        scratch = [pltpu.VMEM((layers, *s), jnp.bfloat16) for s in shapes]
        scratch += [pltpu.VMEM((2, terms_kept, *s), jnp.bfloat16) for s in shapes]
        scratch += [pltpu.VMEM((2, sums, *s), jnp.bfloat16) for s in shapes]
        scratch += [pltpu.VMEM((n, 8, 128), jnp.float32)]
        scratch += [dma((2, sums, 3)), dma((3,)), dma((2,)), dma((1,)), dma((1,)), dma((3,)), dma((3,)), dma((3, 3))]
        in_vmem, in_hbm = pl.BlockSpec(memory_space=pltpu.VMEM), pl.BlockSpec(memory_space=pltpu.HBM)
        new = [*weights[:2], jax.ShapeDtypeStruct(m[2].shape, weights[2].dtype), *m, *v]
        new = pl.pallas_call(
            functools.partial(sum_and_step, n, layers, count),
            out_shape=[pltpu.VMEM(one.shape, one.dtype) for one in new],
            in_specs=[in_hbm] * 12,
            out_specs=[in_vmem] * 9,
            scratch_shapes=scratch,
            compiler_params=pltpu.CompilerParams(collective_id=0, has_side_effects=True, vmem_limit_bytes=40 * 2**20),
        )(*terms, *weights, *m, *v)

        def written(*kept):
            return pl.pallas_call(
                write_out,
                out_shape=[*(jax.ShapeDtypeStruct(one.shape, one.dtype) for one in kept), pltpu.VMEM((8, 128), jnp.float32)],
                in_specs=[in_vmem] * len(kept),
                out_specs=[in_hbm] * len(kept) + [in_vmem],
                scratch_shapes=[dma((len(kept),))],
                compiler_params=pltpu.CompilerParams(vmem_limit_bytes=2**20),
            )(*kept)

        gate, up, *moments, done = written(*new[:2], *new[3:])
        down = pl.pallas_call(
            functools.partial(gather_last, n),
            out_shape=pltpu.VMEM(weights[2].shape, weights[2].dtype),
            in_specs=[in_vmem, in_vmem],
            out_specs=in_vmem,
            scratch_shapes=[dma((2, sums, 1)), dma((1,))],
            compiler_params=pltpu.CompilerParams(collective_id=1, has_side_effects=True, vmem_limit_bytes=2**20),
        )(new[2], done)
        return (gate, up, down, *moments)

    all_of, cut = P(None, None, None), P(None, "dp", None)
    return jax.shard_map(
        step,
        mesh=mesh,
        in_specs=(P(("rep", "dp"), None, None, None),) * 3 + (all_of,) * 3 + (cut,) * 6,
        out_specs=(P("rep", None, None),) * 3 + (P("rep", "dp", None),) * 6,
        check_vma=False,
    )
```

```python
import functools

import jax
import jax.numpy as jnp
from jax import lax
from jax.experimental import pallas as pl
from jax.experimental.pallas import tpu as pltpu
from jax.sharding import PartitionSpec as P

WAYS = (1, -1)
LAG_NS = 6000


def row_blocks(rows, columns):
    best = 16
    for step in range(16, rows + 1, 16):
        if rows % step == 0 and step * columns <= 32 * 1024:
            best = step
    return best


def remote(src, dst, send, recv, to):
    return pltpu.make_async_remote_copy(src, dst, send, recv, device_id={"dp": to}, device_id_type=pl.DeviceIdType.MESH)


def meet(n):
    me = lax.axis_index("dp")

    def at(way, steps):
        return lax.rem(me + WAYS[way] * steps + n, n)

    barrier = pltpu.get_barrier_semaphore()
    for way in range(2):
        pl.semaphore_signal(barrier, inc=1, device_id={"dp": at(way, 1)}, device_id_type=pl.DeviceIdType.MESH)
    pl.semaphore_wait(barrier, 2)
    return me, at


def halved(layers, way):
    return range(way * layers // 2, (way + 1) * layers // 2)


class Gather:
    def __init__(self, n, at, outs, rows, arrived, sent):
        self.half, self.at, self.outs, self.rows, self.arrived, self.sent = n // 2, at, outs, rows, arrived, sent
        self.n, self.layers, self.copies = n, outs[0].shape[0], {}

    def block(self, chunk, kind):
        return pl.ds(pl.multiple_of(chunk * self.rows[kind], 16), self.rows[kind])

    def send(self, way, step, layer, kind, src=None):
        here = self.outs[kind].at[layer, self.block(self.at(way, 1 - step), kind)]
        slot = (step - 1) * self.layers + (layer if step < self.half else layer - halved(self.layers, way)[0])
        copy = remote(here if src is None else src, here, self.sent.at[kind], self.arrived.at[way, slot, kind], self.at(way, 1))
        self.copies[way, step, layer, kind] = copy
        copy.start()

    def run(self):
        for step in range(1, self.half + 1):
            for i in range(self.layers):
                for kind in range(len(self.outs)):
                    for way in range(2):
                        far = halved(self.layers, way)
                        layer = (*far, *halved(self.layers, 1 - way))[i]
                        if step == self.half and layer not in far:
                            continue
                        self.copies[way, step, layer, kind].wait_recv()
                        if step < self.half - 1 or (step == self.half - 1 and layer in far):
                            self.send(way, step + 1, layer, kind)
        for kind, out in enumerate(self.outs):
            moved = out.at[:, pl.ds(0, (self.n - 1) * self.rows[kind])]
            pltpu.make_async_copy(moved, moved, self.sent.at[kind]).wait()


def sum_and_step(n, layers, count, *refs):
    kinds = 3
    g, w, m, v = (refs[i : i + kinds] for i in range(0, 4 * kinds, kinds))
    refs = refs[4 * kinds :]
    new_w, new_m, new_v = (refs[i : i + kinds] for i in range(0, 3 * kinds, kinds))
    refs = refs[3 * kinds :]
    own, term, got = (refs[i : i + kinds] for i in range(0, 3 * kinds, kinds))
    squares, arrived, rs_send, ag_send, sq_send, sq_recv, load_own, load_term, load_state = refs[3 * kinds :]
    half = n // 2
    rows = [ref.shape[1] for ref in own]
    pairs = [(layer, kind) for kind in range(kinds) for layer in range(layers)]
    me, at = meet(n)

    def block(chunk, kind):
        return pl.ds(pl.multiple_of(chunk * rows[kind], 16), rows[kind])

    def slot(step, layer, way):
        return layer - halved(layers, way)[0] if step == 1 else layers // 2 + (step - 2) * layers + layer

    def term_slot(step, layer, way):
        return layer - halved(layers, way)[0] if step == 2 else layers // 2 + (step - 3) * layers + layer

    sums = {}

    def send_sum(way, step, layer, kind, src):
        here = slot(step, layer, way)
        sems = (rs_send.at[kind], arrived.at[way, here, kind])
        sums[way, step, layer, kind] = remote(src, got[kind].at[way, here], *sems, at(way, 1))
        sums[way, step, layer, kind].start()

    def fetch():
        for kind in range(kinds):
            for step in range(2, half + 1):
                for way in range(2):
                    first = halved(layers, way)[0] if step == 2 else 0
                    many = layers // 2 if step == 2 else layers
                    src = g[kind].at[pl.ds(first, many), block(at(way, half + 1 - step), kind)]
                    dst = term[kind].at[way, pl.ds(term_slot(step, first, way), many)]
                    pltpu.make_async_copy(src, dst, load_term.at[kind]).start()
        copies = []
        for kind in range(kinds):
            here = block(me, kind)
            copies.append(pltpu.make_async_copy(g[kind].at[:, here], own[kind], load_own.at[kind]))
            copies.append(pltpu.make_async_copy(m[kind], new_m[kind], load_state.at[0, kind]))
            copies.append(pltpu.make_async_copy(v[kind], new_v[kind], load_state.at[1, kind]))
            to = new_w[kind].at[:, here] if kind < kinds - 1 else new_w[kind]
            copies.append(pltpu.make_async_copy(w[kind].at[:, here], to, load_state.at[2, kind]))
        for copy in copies:
            copy.start()
        for kind in range(kinds):
            pltpu.make_async_copy(term[kind], term[kind], load_term.at[kind]).wait()
        for copy in copies:
            copy.wait()

    late = lax.rem(lax.axis_index("rep"), 2) == 0

    @pl.when(late)
    def _():
        fetch()
        pl.delay(LAG_NS)

    for kind in range(kinds):
        for i in range(layers // 2):
            for way in range(2):
                layer = halved(layers, way)[i]
                send_sum(way, 1, layer, kind, g[kind].at[layer, block(at(way, half), kind)])
    for kind in range(kinds):
        for i in range(layers // 2):
            for way in range(2):
                layer = halved(layers, 1 - way)[i]
                send_sum(way, 2, layer, kind, g[kind].at[layer, block(at(way, half - 1), kind)])

    @pl.when(jnp.logical_not(late))
    def _():
        fetch()

    def each_rows(kind, body, carry=None):
        many = row_blocks(rows[kind], own[kind].shape[2])

        def one(i, carry):
            return body(pl.ds(pl.multiple_of(i * many, many), many), carry)

        return lax.fori_loop(0, rows[kind] // many, one, carry)

    def pass_on(way, step, layer, kind):
        sums[way, step - 1, layer, kind].wait_recv()
        into = got[kind].at[way, slot(step - 1, layer, way)]
        mine = term[kind].at[way, term_slot(step, layer, way)]

        def add(r, _):
            into[r] = (into[r].astype(jnp.float32) + mine[r].astype(jnp.float32)).astype(jnp.bfloat16)

        each_rows(kind, add)
        send_sum(way, step, layer, kind, into)

    for kind in range(kinds):
        for i in range(layers // 2):
            for way in range(2):
                pass_on(way, 2, halved(layers, way)[i], kind)
    for step in range(3, half + 1):
        for j in range(layers):
            for kind in range(kinds):
                for way in range(2):
                    order = (*halved(layers, 1 - way), *halved(layers, way)) if step < half else range(layers)
                    pass_on(way, step, order[j], kind)

    total = jnp.zeros((8, 128), jnp.float32)
    for layer, kind in pairs:
        for way in range(2):
            sums[way, half, layer, kind].wait_recv()
        ends = [got[kind].at[way, slot(half, layer, way)] for way in range(2)]
        mine = own[kind].at[layer]

        def finish(r, total):
            x = mine[r].astype(jnp.float32) + ends[0][r].astype(jnp.float32) + ends[1][r].astype(jnp.float32)
            x = x.astype(jnp.bfloat16)
            mine[r] = x
            x = x.astype(jnp.float32)
            x = x * x
            parts = [x[i : i + 8, j : j + 128] for i in range(0, x.shape[0], 8) for j in range(0, x.shape[1], 128)]
            while len(parts) > 1:
                parts = [a + b for a, b in zip(parts[::2], parts[1::2])] + ([parts[-1]] if len(parts) % 2 else [])
            return total + parts[0]

        total = each_rows(kind, finish, total)

    squares[me] = jnp.sum(total, axis=0, keepdims=True)
    told = []
    for off in range(1, n):
        told.append(remote(squares.at[me], squares.at[me], sq_send.at[0], sq_recv.at[0], lax.rem(me + off, n)))
        told[-1].start()
    others = squares.at[pl.ds(0, n - 1)]
    pltpu.make_async_copy(others, others, sq_recv.at[0]).wait()
    total = jnp.sum(jnp.sum(squares[...], axis=0), axis=1, keepdims=True)
    factor = jnp.minimum(1.0, 0.5 * lax.rsqrt(total / count + 1e-30))

    gather = Gather(n, at, new_w[: kinds - 1], rows, arrived, ag_send)
    for kind in range(kinds):
        for layer in range(layers):
            grad, m_at, v_at = own[kind].at[layer], new_m[kind].at[layer], new_v[kind].at[layer]
            base = pl.multiple_of(me * rows[kind], 16) if kind < kinds - 1 else 0
            w_at = new_w[kind].at[layer]

            def adamw(r, _):
                x = grad[r].astype(jnp.float32) * factor
                there = pl.ds(pl.multiple_of(base + r.start, 16), r.size)
                old = w_at[there].astype(jnp.float32)
                m_new = 0.9 * m_at[r] + 0.1 * x
                v_new = 0.95 * v_at[r] + 0.05 * x * x
                m_at[r] = m_new
                v_at[r] = v_new
                step = m_new * lax.rsqrt(v_new + 1e-8) + 0.1 * old
                w_at[there] = (old - 0.02 * step).astype(jnp.bfloat16)

            each_rows(kind, adamw)
            if kind < kinds - 1:
                for way in range(2):
                    gather.send(way, 1, layer, kind)
    gather.run()
    for kind in range(kinds):
        pltpu.make_async_copy(got[kind], got[kind], rs_send.at[kind]).wait()
    pltpu.make_async_copy(others, others, sq_send.at[0]).wait()


def gather_last(n, own, after, out, arrived, sent):
    me, at = meet(n)
    gather = Gather(n, at, [out], [own.shape[1]], arrived, sent)
    for i in range(own.shape[0]):
        for way in range(2):
            layer = (*halved(own.shape[0], way), *halved(own.shape[0], 1 - way))[i]
            gather.send(way, 1, layer, 0, own.at[layer])
    out[:, gather.block(me, 0)] = own[...]
    gather.run()


def write_out(*refs):
    n = (len(refs) - 2) // 2
    copies = [pltpu.make_async_copy(src, dst, refs[-1].at[i]) for i, (src, dst) in enumerate(zip(refs[:n], refs[n : 2 * n]))]
    refs[-2][...] = jnp.zeros_like(refs[-2])
    for copy in copies:
        copy.start()
    for copy in copies:
        copy.wait()


def solution(mesh):
    n = mesh.shape["dp"]

    def step(*arrays):
        terms, weights, m, v = (arrays[i : i + 3] for i in (0, 3, 6, 9))
        terms = [t[0] for t in terms]
        layers = m[0].shape[0]
        shapes = [one.shape[1:] for one in m]
        count = n * sum(one.size for one in m)
        half = n // 2
        sums = layers // 2 + (half - 1) * layers
        terms_kept = layers // 2 + (half - 2) * layers
        dma = pltpu.SemaphoreType.DMA
        scratch = [pltpu.VMEM((layers, *s), jnp.bfloat16) for s in shapes]
        scratch += [pltpu.VMEM((2, terms_kept, *s), jnp.bfloat16) for s in shapes]
        scratch += [pltpu.VMEM((2, sums, *s), jnp.bfloat16) for s in shapes]
        scratch += [pltpu.VMEM((n, 1, 128), jnp.float32)]
        scratch += [dma((2, sums, 3)), dma((3,)), dma((2,)), dma((1,)), dma((1,)), dma((3,)), dma((3,)), dma((3, 3))]
        in_vmem, in_hbm = pl.BlockSpec(memory_space=pltpu.VMEM), pl.BlockSpec(memory_space=pltpu.HBM)
        new = [*weights[:2], jax.ShapeDtypeStruct(m[2].shape, weights[2].dtype), *m, *v]
        new = pl.pallas_call(
            functools.partial(sum_and_step, n, layers, count),
            out_shape=[pltpu.VMEM(one.shape, one.dtype) for one in new],
            in_specs=[in_hbm] * 12,
            out_specs=[in_vmem] * 9,
            scratch_shapes=scratch,
            compiler_params=pltpu.CompilerParams(collective_id=0, has_side_effects=True, vmem_limit_bytes=40 * 2**20),
        )(*terms, *weights, *m, *v)

        def written(*kept):
            return pl.pallas_call(
                write_out,
                out_shape=[*(jax.ShapeDtypeStruct(one.shape, one.dtype) for one in kept), pltpu.VMEM((8, 128), jnp.float32)],
                in_specs=[in_vmem] * len(kept),
                out_specs=[in_hbm] * len(kept) + [in_vmem],
                scratch_shapes=[dma((len(kept),))],
                compiler_params=pltpu.CompilerParams(vmem_limit_bytes=2**20),
            )(*kept)

        gate, up, *moments, done = written(*new[:2], *new[3:])
        down = pl.pallas_call(
            functools.partial(gather_last, n),
            out_shape=pltpu.VMEM(weights[2].shape, weights[2].dtype),
            in_specs=[in_vmem, in_vmem],
            out_specs=in_vmem,
            scratch_shapes=[dma((2, sums, 1)), dma((1,))],
            compiler_params=pltpu.CompilerParams(collective_id=1, has_side_effects=True, vmem_limit_bytes=2**20),
        )(new[2], done)
        return (gate, up, down, *moments)

    all_of, cut = P(None, None, None), P(None, "dp", None)
    return jax.shard_map(
        step,
        mesh=mesh,
        in_specs=(P(("rep", "dp"), None, None, None),) * 3 + (all_of,) * 3 + (cut,) * 6,
        out_specs=(P("rep", None, None),) * 3 + (P("rep", "dp", None),) * 6,
        check_vma=False,
    )
```

```python
import functools

import jax
import jax.numpy as jnp
from jax import lax
from jax.experimental import pallas as pl
from jax.experimental.pallas import tpu as pltpu
from jax.sharding import PartitionSpec as P

WAYS = (1, -1)
LAG_NS = 4000
PAUSE_NS = 11700


def row_blocks(rows, columns):
    best = 16
    for step in range(16, rows + 1, 16):
        if rows % step == 0 and step * columns <= 32 * 1024:
            best = step
    return best


def remote(src, dst, send, recv, to):
    return pltpu.make_async_remote_copy(src, dst, send, recv, device_id={"dp": to}, device_id_type=pl.DeviceIdType.MESH)


def ring(n):
    me = lax.axis_index("dp")
    return me, lambda way, steps: lax.rem(me + WAYS[way] * steps + n, n)


def meet(at):
    barrier = pltpu.get_barrier_semaphore()
    for way in range(2):
        pl.semaphore_signal(barrier, inc=1, device_id={"dp": at(way, 1)}, device_id_type=pl.DeviceIdType.MESH)
    pl.semaphore_wait(barrier, 2)


def halved(layers, way):
    return range(way * layers // 2, (way + 1) * layers // 2)


def ends_last():
    return lax.rem(lax.axis_index("rep"), 2) == 0


class Gather:
    def __init__(self, n, at, outs, rows, orders, arrived, sent):
        self.n, self.half, self.at, self.outs, self.rows, self.orders = n, n // 2, at, outs, rows, orders
        self.arrived, self.sent = arrived, sent

    def order(self, way, step):
        return [piece for piece in self.orders[way] if step < self.half or piece[4] == way]

    def copy(self, way, step, piece, src=None):
        kind, layer, first, many, _ = piece
        here = self.outs[kind].at[layer, pl.ds(pl.multiple_of(self.at(way, 1 - step) * self.rows[kind] + first, 16), many)]
        arrived = self.arrived.at[way, (step - 1) * len(self.orders[way]) + self.order(way, step).index(piece)]
        return remote(here if src is None else src, here, self.sent.at[kind], arrived, self.at(way, 1))

    def run(self, short=()):
        for step in range(1, self.half + 1):
            for i in range(len(self.orders[0])):
                for way in range(2):
                    for piece in self.order(way, step)[i : i + 1]:
                        if step == self.half and piece[0] in short:
                            continue
                        self.copy(way, step, piece).wait_recv()
                        if step < self.half and piece in self.order(way, step + 1) and not (step + 1 == self.half and piece[0] in short):
                            self.copy(way, step + 1, piece).start()
        for kind in sorted({piece[0] for piece in self.orders[0]}):
            blocks = self.n - 2 if kind in short else self.n - 1
            self.wait_sent(kind, blocks)

    def wait_sent(self, kind, blocks):
        moved = self.outs[kind].at[:, pl.ds(0, blocks * self.rows[kind])]
        pltpu.make_async_copy(moved, moved, self.sent.at[kind]).wait()


def sum_and_step(n, layers, count, *refs):
    kinds = 3
    g, w, m, v = (refs[i : i + kinds] for i in range(0, 4 * kinds, kinds))
    refs = refs[4 * kinds :]
    new_w, new_m, new_v = (refs[i : i + kinds] for i in range(0, 3 * kinds, kinds))
    refs = refs[3 * kinds :]
    own, term, got = (refs[i : i + kinds] for i in range(0, 3 * kinds, kinds))
    squares, arrived, rs_send, ag_send, sq_send, sq_recv, load_own, load_term, load_state = refs[3 * kinds :]
    half = n // 2
    rows = [ref.shape[1] for ref in own]
    pairs = [(layer, kind) for kind in range(kinds) for layer in range(layers)]
    me, at = ring(n)
    meet(at)

    def block(chunk, kind):
        return pl.ds(pl.multiple_of(chunk * rows[kind], 16), rows[kind])

    def slot(step, layer, way):
        return layer - halved(layers, way)[0] if step == 1 else layers // 2 + (step - 2) * layers + layer

    def term_slot(step, layer, way):
        return layer - halved(layers, way)[0] if step == 2 else layers // 2 + (step - 3) * layers + layer

    sums = {}

    def send_sum(way, step, layer, kind, src):
        here = slot(step, layer, way)
        sems = (rs_send.at[kind], arrived.at[way, here * kinds + kind])
        sums[way, step, layer, kind] = remote(src, got[kind].at[way, here], *sems, at(way, 1))
        sums[way, step, layer, kind].start()

    def fetch():
        for kind in range(kinds):
            for step in range(2, half + 1):
                for way in range(2):
                    first = halved(layers, way)[0] if step == 2 else 0
                    many = layers // 2 if step == 2 else layers
                    src = g[kind].at[pl.ds(first, many), block(at(way, half + 1 - step), kind)]
                    dst = term[kind].at[way, pl.ds(term_slot(step, first, way), many)]
                    pltpu.make_async_copy(src, dst, load_term.at[kind]).start()
        copies = []
        for kind in range(kinds):
            here = block(me, kind)
            copies.append(pltpu.make_async_copy(g[kind].at[:, here], own[kind], load_own.at[kind]))
            copies.append(pltpu.make_async_copy(m[kind], new_m[kind], load_state.at[0, kind]))
            copies.append(pltpu.make_async_copy(v[kind], new_v[kind], load_state.at[1, kind]))
            copies.append(pltpu.make_async_copy(w[kind].at[:, here], new_w[kind].at[:, here], load_state.at[2, kind]))
        for copy in copies:
            copy.start()
        for kind in range(kinds):
            pltpu.make_async_copy(term[kind], term[kind], load_term.at[kind]).wait()
        for copy in copies:
            copy.wait()

    late = ends_last()

    @pl.when(late)
    def _():
        fetch()
        pl.delay(LAG_NS)

    for kind in range(kinds):
        for i in range(layers // 2):
            for way in range(2):
                layer = halved(layers, way)[i]
                send_sum(way, 1, layer, kind, g[kind].at[layer, block(at(way, half), kind)])
    for kind in range(kinds):
        for i in range(layers // 2):
            for way in range(2):
                layer = halved(layers, 1 - way)[i]
                send_sum(way, 2, layer, kind, g[kind].at[layer, block(at(way, half - 1), kind)])

    @pl.when(jnp.logical_not(late))
    def _():
        fetch()

    def each_rows(kind, body, carry=None):
        many = row_blocks(rows[kind], own[kind].shape[2])

        def one(i, carry):
            return body(pl.ds(pl.multiple_of(i * many, many), many), carry)

        return lax.fori_loop(0, rows[kind] // many, one, carry)

    def pass_on(way, step, layer, kind):
        sums[way, step - 1, layer, kind].wait_recv()
        into = got[kind].at[way, slot(step - 1, layer, way)]
        mine = term[kind].at[way, term_slot(step, layer, way)]

        def add(r, _):
            into[r] = (into[r].astype(jnp.float32) + mine[r].astype(jnp.float32)).astype(jnp.bfloat16)

        each_rows(kind, add)
        send_sum(way, step, layer, kind, into)

    for kind in range(kinds):
        for i in range(layers // 2):
            for way in range(2):
                pass_on(way, 2, halved(layers, way)[i], kind)
    for step in range(3, half + 1):
        for j in range(layers):
            for kind in range(kinds):
                for way in range(2):
                    order = (*halved(layers, 1 - way), *halved(layers, way)) if step < half else range(layers)
                    pass_on(way, step, order[j], kind)

    total = jnp.zeros((8, 128), jnp.float32)
    for layer, kind in pairs:
        for way in range(2):
            sums[way, half, layer, kind].wait_recv()
        ends = [got[kind].at[way, slot(half, layer, way)] for way in range(2)]
        mine = own[kind].at[layer]

        def finish(r, total):
            x = mine[r].astype(jnp.float32) + ends[0][r].astype(jnp.float32) + ends[1][r].astype(jnp.float32)
            x = x.astype(jnp.bfloat16)
            mine[r] = x
            x = x.astype(jnp.float32)
            x = x * x
            parts = [x[i : i + 8, j : j + 128] for i in range(0, x.shape[0], 8) for j in range(0, x.shape[1], 128)]
            while len(parts) > 1:
                parts = [a + b for a, b in zip(parts[::2], parts[1::2])] + ([parts[-1]] if len(parts) % 2 else [])
            return total + parts[0]

        total = each_rows(kind, finish, total)

    squares[me] = jnp.sum(total, axis=0, keepdims=True)
    told = []
    for off in range(1, n):
        told.append(remote(squares.at[me], squares.at[me], sq_send.at[0], sq_recv.at[0], lax.rem(me + off, n)))
        told[-1].start()
    others = squares.at[pl.ds(0, n - 1)]
    pltpu.make_async_copy(others, others, sq_recv.at[0]).wait()
    total = jnp.sum(jnp.sum(squares[...], axis=0), axis=1, keepdims=True)
    factor = jnp.minimum(1.0, 0.5 * lax.rsqrt(total / count + 1e-30))

    pieces = [[(kind, layer, 0, rows[kind], layer * 2 // layers) for kind in range(kinds)] for layer in range(layers)]
    some = Gather(n, at, new_w, rows, [sum((one[:-1] for one in pieces[::step]), []) for step in WAYS], arrived, ag_send)
    more = Gather(n, at, new_w, rows, [sum(pieces[::step], []) for step in WAYS], arrived, ag_send)
    for kind in range(kinds):
        for layer in range(layers):
            grad, m_at, v_at = own[kind].at[layer], new_m[kind].at[layer], new_v[kind].at[layer]
            base = pl.multiple_of(me * rows[kind], 16)
            w_at = new_w[kind].at[layer]

            def adamw(r, _):
                x = grad[r].astype(jnp.float32) * factor
                there = pl.ds(pl.multiple_of(base + r.start, 16), r.size)
                old = w_at[there].astype(jnp.float32)
                m_new = 0.9 * m_at[r] + 0.1 * x
                v_new = 0.95 * v_at[r] + 0.05 * x * x
                m_at[r] = m_new
                v_at[r] = v_new
                step = m_new * lax.rsqrt(v_new + 1e-8) + 0.1 * old
                w_at[there] = (old - 0.02 * step).astype(jnp.bfloat16)

            each_rows(kind, adamw)
            @pl.when(late)
            def _():
                for way in range(2):
                    more.copy(way, 1, pieces[layer][kind]).start()

            if kind < kinds - 1:

                @pl.when(jnp.logical_not(late))
                def _():
                    for way in range(2):
                        some.copy(way, 1, pieces[layer][kind]).start()

    @pl.when(late)
    def _():
        more.run(short=(kinds - 1,))

    @pl.when(jnp.logical_not(late))
    def _():
        some.run()

    for kind in range(kinds):
        pltpu.make_async_copy(got[kind], got[kind], rs_send.at[kind]).wait()
    pltpu.make_async_copy(others, others, sq_send.at[0]).wait()


def gather_last(n, begun, after, rest, arrived, sent):
    me, at = ring(n)
    late = ends_last()

    @pl.when(jnp.logical_not(late))
    def _():
        pl.delay(PAUSE_NS)

    meet(at)
    layers, rows = begun.shape[0], begun.shape[1] // n
    pieces = [(0, layer, 0, rows, layer * 2 // layers) for layer in range(layers)]
    gather = Gather(n, at, [rest], [rows], [pieces[::step] for step in WAYS], arrived, sent)

    def source(way, steps, layer):
        return begun.at[layer, pl.ds(pl.multiple_of(at(way, -steps) * rows, 16), rows)]

    @pl.when(late)
    def _():
        for way in range(2):
            for piece in gather.order(way, n // 2):
                gather.copy(way, n // 2, piece, source(way, n // 2 - 1, piece[1])).start()
        for way in range(2):
            for piece in gather.order(way, n // 2):
                gather.copy(way, n // 2, piece).wait_recv()
        gather.wait_sent(0, 1)

    @pl.when(jnp.logical_not(late))
    def _():
        for i in range(layers):
            for way in range(2):
                gather.copy(way, 1, gather.orders[way][i], source(way, 0, gather.orders[way][i][1])).start()
        gather.run()


def copy_blocks(n, src, dst, sem, offsets):
    me, at = ring(n)
    rows = src.shape[1] // n
    blocks = [pl.ds(pl.multiple_of(at(0, off) * rows, 16), rows) for off in offsets]
    return [pltpu.make_async_copy(src.at[:, here], dst.at[:, here], sem.at[off]) for here, off in zip(blocks, offsets)]


def run_all(copies):
    for copy in copies:
        copy.start()
    for copy in copies:
        copy.wait()


def write_most(n, *refs):
    *refs, done, sems, block_sems = refs
    whole = [pltpu.make_async_copy(src, dst, sems.at[i]) for i, (src, dst) in enumerate(zip(refs[:9], refs[9:])) if i != 2]
    for copy in whole:
        copy.start()
    done[...] = jnp.zeros_like(done)
    late = ends_last()

    @pl.when(late)
    def _():
        run_all(copy_blocks(n, refs[2], refs[11], block_sems, [off for off in range(n) if off != n // 2]))

    @pl.when(jnp.logical_not(late))
    def _():
        run_all(copy_blocks(n, refs[2], refs[11], block_sems, [0]))

    for copy in whole:
        copy.wait()


def write_rest(n, rest, begun, out, sems):
    late = ends_last()

    @pl.when(late)
    def _():
        run_all(copy_blocks(n, rest, out, sems, [n // 2]))

    @pl.when(jnp.logical_not(late))
    def _():
        run_all(copy_blocks(n, rest, out, sems, range(1, n)))


def solution(mesh):
    n = mesh.shape["dp"]

    def step(*arrays):
        terms, weights, m, v = (arrays[i : i + 3] for i in (0, 3, 6, 9))
        terms = [t[0] for t in terms]
        layers = m[0].shape[0]
        shapes = [one.shape[1:] for one in m]
        count = n * sum(one.size for one in m)
        half = n // 2
        sums = layers // 2 + (half - 1) * layers
        terms_kept = layers // 2 + (half - 2) * layers
        dma = pltpu.SemaphoreType.DMA
        scratch = [pltpu.VMEM((layers, *s), jnp.bfloat16) for s in shapes]
        scratch += [pltpu.VMEM((2, terms_kept, *s), jnp.bfloat16) for s in shapes]
        scratch += [pltpu.VMEM((2, sums, *s), jnp.bfloat16) for s in shapes]
        scratch += [pltpu.VMEM((n, 1, 128), jnp.float32)]
        scratch += [dma((2, 3 * sums)), dma((3,)), dma((3,)), dma((1,)), dma((1,)), dma((3,)), dma((3,)), dma((3, 3))]
        in_vmem, in_hbm = pl.BlockSpec(memory_space=pltpu.VMEM), pl.BlockSpec(memory_space=pltpu.HBM)
        new = [*weights, *m, *v]
        kept = pl.pallas_call(
            functools.partial(sum_and_step, n, layers, count),
            out_shape=[pltpu.VMEM(one.shape, one.dtype) for one in new],
            in_specs=[in_hbm] * 12,
            out_specs=[in_vmem] * 9,
            scratch_shapes=scratch,
            compiler_params=pltpu.CompilerParams(collective_id=0, has_side_effects=True, vmem_limit_bytes=40 * 2**20),
        )(*terms, *weights, *m, *v)
        *written, done = pl.pallas_call(
            functools.partial(write_most, n),
            out_shape=[*(jax.ShapeDtypeStruct(one.shape, one.dtype) for one in new), pltpu.VMEM((8, 128), jnp.float32)],
            in_specs=[in_vmem] * 9,
            out_specs=[in_hbm] * 9 + [in_vmem],
            scratch_shapes=[dma((9,)), dma((n,))],
            compiler_params=pltpu.CompilerParams(vmem_limit_bytes=2**20),
        )(*kept)
        rest = pl.pallas_call(
            functools.partial(gather_last, n),
            out_shape=pltpu.VMEM(weights[2].shape, weights[2].dtype),
            in_specs=[in_vmem, in_vmem],
            out_specs=in_vmem,
            scratch_shapes=[dma((2, half * layers)), dma((1,))],
            compiler_params=pltpu.CompilerParams(collective_id=1, has_side_effects=True, vmem_limit_bytes=2**20),
        )(kept[2], done)
        written[2] = pl.pallas_call(
            functools.partial(write_rest, n),
            out_shape=jax.ShapeDtypeStruct(weights[2].shape, weights[2].dtype),
            in_specs=[in_vmem, in_hbm],
            out_specs=in_hbm,
            input_output_aliases={1: 0},
            scratch_shapes=[dma((n,))],
            compiler_params=pltpu.CompilerParams(vmem_limit_bytes=2**20),
        )(rest, written[2])
        return tuple(written)

    all_of, cut = P(None, None, None), P(None, "dp", None)
    return jax.shard_map(
        step,
        mesh=mesh,
        in_specs=(P(("rep", "dp"), None, None, None),) * 3 + (all_of,) * 3 + (cut,) * 6,
        out_specs=(P("rep", None, None),) * 3 + (P("rep", "dp", None),) * 6,
        check_vma=False,
    )
```

```python
import functools

import jax
import jax.numpy as jnp
from jax import lax
from jax.experimental import pallas as pl
from jax.experimental.pallas import tpu as pltpu
from jax.sharding import PartitionSpec as P

WAYS = (1, -1)
LAG_NS = 4000
PAUSE_NS = 11500


def row_blocks(rows, columns):
    best = 16
    for step in range(16, rows + 1, 16):
        if rows % step == 0 and step * columns <= 32 * 1024:
            best = step
    return best


def remote(src, dst, send, recv, to):
    return pltpu.make_async_remote_copy(src, dst, send, recv, device_id={"dp": to}, device_id_type=pl.DeviceIdType.MESH)


def ring(n):
    me = lax.axis_index("dp")
    return me, lambda way, steps: lax.rem(me + WAYS[way] * steps + n, n)


def meet(at):
    barrier = pltpu.get_barrier_semaphore()
    for way in range(2):
        pl.semaphore_signal(barrier, inc=1, device_id={"dp": at(way, 1)}, device_id_type=pl.DeviceIdType.MESH)
    pl.semaphore_wait(barrier, 2)


def halved(layers, way):
    return range(way * layers // 2, (way + 1) * layers // 2)


def ends_last():
    return lax.rem(lax.axis_index("rep"), 2) == 0


class Gather:
    def __init__(self, n, at, outs, rows, orders, arrived, sent):
        self.n, self.half, self.at, self.outs, self.rows, self.orders = n, n // 2, at, outs, rows, orders
        self.arrived, self.sent = arrived, sent

    def order(self, way, step):
        return [piece for piece in self.orders[way] if step < self.half or piece[4] == way]

    def copy(self, way, step, piece, src=None):
        kind, layer, first, many, _ = piece
        here = self.outs[kind].at[layer, pl.ds(pl.multiple_of(self.at(way, 1 - step) * self.rows[kind] + first, 16), many)]
        arrived = self.arrived.at[way, (step - 1) * len(self.orders[way]) + self.order(way, step).index(piece)]
        return remote(here if src is None else src, here, self.sent.at[kind], arrived, self.at(way, 1))

    def run(self, short=()):
        for step in range(1, self.half + 1):
            for i in range(len(self.orders[0])):
                for way in range(2):
                    for piece in self.order(way, step)[i : i + 1]:
                        if step == self.half and piece[0] in short:
                            continue
                        self.copy(way, step, piece).wait_recv()
                        if step < self.half and piece in self.order(way, step + 1) and not (step + 1 == self.half and piece[0] in short):
                            self.copy(way, step + 1, piece).start()
        for kind in sorted({piece[0] for piece in self.orders[0]}):
            blocks = self.n - 2 if kind in short else self.n - 1
            self.wait_sent(kind, blocks)

    def wait_sent(self, kind, blocks):
        moved = self.outs[kind].at[:, pl.ds(0, blocks * self.rows[kind])]
        pltpu.make_async_copy(moved, moved, self.sent.at[kind]).wait()


def sum_and_step(n, layers, count, *refs):
    kinds = 3
    g, w, m, v = (refs[i : i + kinds] for i in range(0, 4 * kinds, kinds))
    refs = refs[4 * kinds :]
    new_w, new_m, new_v = (refs[i : i + kinds] for i in range(0, 3 * kinds, kinds))
    refs = refs[3 * kinds :]
    own, term, got = (refs[i : i + kinds] for i in range(0, 3 * kinds, kinds))
    squares, arrived, rs_send, ag_send, sq_send, sq_recv, load_own, load_term, load_state = refs[3 * kinds :]
    half = n // 2
    rows = [ref.shape[1] for ref in own]
    pairs = [(layer, kind) for kind in range(kinds) for layer in range(layers)]
    me, at = ring(n)
    meet(at)

    def block(chunk, kind):
        return pl.ds(pl.multiple_of(chunk * rows[kind], 16), rows[kind])

    def slot(step, layer, way):
        return layer - halved(layers, way)[0] if step == 1 else layers // 2 + (step - 2) * layers + layer

    def term_slot(step, layer, way):
        return layer - halved(layers, way)[0] if step == 2 else layers // 2 + (step - 3) * layers + layer

    sums = {}

    def send_sum(way, step, layer, kind, src):
        here = slot(step, layer, way)
        sems = (rs_send.at[kind], arrived.at[way, here * kinds + kind])
        sums[way, step, layer, kind] = remote(src, got[kind].at[way, here], *sems, at(way, 1))
        sums[way, step, layer, kind].start()

    def fetch():
        for kind in range(kinds):
            for step in range(2, half + 1):
                for way in range(2):
                    first = halved(layers, way)[0] if step == 2 else 0
                    many = layers // 2 if step == 2 else layers
                    src = g[kind].at[pl.ds(first, many), block(at(way, half + 1 - step), kind)]
                    dst = term[kind].at[way, pl.ds(term_slot(step, first, way), many)]
                    pltpu.make_async_copy(src, dst, load_term.at[kind]).start()
        copies = []
        for kind in range(kinds):
            here = block(me, kind)
            copies.append(pltpu.make_async_copy(g[kind].at[:, here], own[kind], load_own.at[kind]))
            copies.append(pltpu.make_async_copy(m[kind], new_m[kind], load_state.at[0, kind]))
            copies.append(pltpu.make_async_copy(v[kind], new_v[kind], load_state.at[1, kind]))
            copies.append(pltpu.make_async_copy(w[kind].at[:, here], new_w[kind].at[:, here], load_state.at[2, kind]))
        for copy in copies:
            copy.start()
        for kind in range(kinds):
            pltpu.make_async_copy(term[kind], term[kind], load_term.at[kind]).wait()
        for copy in copies:
            copy.wait()

    late = ends_last()

    @pl.when(late)
    def _():
        fetch()
        pl.delay(LAG_NS)

    for kind in range(kinds):
        for i in range(layers // 2):
            for way in range(2):
                layer = halved(layers, way)[i]
                send_sum(way, 1, layer, kind, g[kind].at[layer, block(at(way, half), kind)])
    for kind in range(kinds):
        for i in range(layers // 2):
            for way in range(2):
                layer = halved(layers, 1 - way)[i]
                send_sum(way, 2, layer, kind, g[kind].at[layer, block(at(way, half - 1), kind)])

    @pl.when(jnp.logical_not(late))
    def _():
        fetch()

    def each_rows(kind, body, carry=None):
        many = row_blocks(rows[kind], own[kind].shape[2])

        def one(i, carry):
            return body(pl.ds(pl.multiple_of(i * many, many), many), carry)

        return lax.fori_loop(0, rows[kind] // many, one, carry)

    def pass_on(way, step, layer, kind):
        sums[way, step - 1, layer, kind].wait_recv()
        into = got[kind].at[way, slot(step - 1, layer, way)]
        mine = term[kind].at[way, term_slot(step, layer, way)]

        def add(r, _):
            into[r] = (into[r].astype(jnp.float32) + mine[r].astype(jnp.float32)).astype(jnp.bfloat16)

        each_rows(kind, add)
        send_sum(way, step, layer, kind, into)

    for kind in range(kinds):
        for i in range(layers // 2):
            for way in range(2):
                pass_on(way, 2, halved(layers, way)[i], kind)
    for step in range(3, half + 1):
        for j in range(layers):
            for kind in range(kinds):
                for way in range(2):
                    order = (*halved(layers, 1 - way), *halved(layers, way)) if step < half else range(layers)
                    pass_on(way, step, order[j], kind)

    total = jnp.zeros((8, 128), jnp.float32)
    for layer, kind in pairs:
        for way in range(2):
            sums[way, half, layer, kind].wait_recv()
        ends = [got[kind].at[way, slot(half, layer, way)] for way in range(2)]
        mine = own[kind].at[layer]

        def finish(r, total):
            x = mine[r].astype(jnp.float32) + ends[0][r].astype(jnp.float32) + ends[1][r].astype(jnp.float32)
            x = x.astype(jnp.bfloat16)
            mine[r] = x
            x = x.astype(jnp.float32)
            x = x * x
            parts = [x[i : i + 8, j : j + 128] for i in range(0, x.shape[0], 8) for j in range(0, x.shape[1], 128)]
            while len(parts) > 1:
                parts = [a + b for a, b in zip(parts[::2], parts[1::2])] + ([parts[-1]] if len(parts) % 2 else [])
            return total + parts[0]

        total = each_rows(kind, finish, total)

    squares[me] = jnp.sum(total, axis=0, keepdims=True)
    told = []
    for off in range(1, n):
        told.append(remote(squares.at[me], squares.at[me], sq_send.at[0], sq_recv.at[0], lax.rem(me + off, n)))
        told[-1].start()
    others = squares.at[pl.ds(0, n - 1)]
    pltpu.make_async_copy(others, others, sq_recv.at[0]).wait()
    total = jnp.sum(jnp.sum(squares[...], axis=0), axis=1, keepdims=True)
    factor = jnp.minimum(1.0, 0.5 * lax.rsqrt(total / count + 1e-30))

    pieces = [[(kind, layer, 0, rows[kind], layer * 2 // layers) for kind in range(kinds)] for layer in range(layers)]
    some = Gather(n, at, new_w, rows, [sum((one[:-1] for one in pieces[::step]), []) for step in WAYS], arrived, ag_send)
    more = Gather(n, at, new_w, rows, [sum(pieces[::step], []) for step in WAYS], arrived, ag_send)
    for kind in range(kinds):
        for layer in range(layers):
            grad, m_at, v_at = own[kind].at[layer], new_m[kind].at[layer], new_v[kind].at[layer]
            base = pl.multiple_of(me * rows[kind], 16)
            w_at = new_w[kind].at[layer]

            def adamw(r, _):
                x = grad[r].astype(jnp.float32) * factor
                there = pl.ds(pl.multiple_of(base + r.start, 16), r.size)
                old = w_at[there].astype(jnp.float32)
                m_new = 0.9 * m_at[r] + 0.1 * x
                v_new = 0.95 * v_at[r] + 0.05 * x * x
                m_at[r] = m_new
                v_at[r] = v_new
                step = m_new * lax.rsqrt(v_new + 1e-8) + 0.1 * old
                w_at[there] = (old - 0.02 * step).astype(jnp.bfloat16)

            each_rows(kind, adamw)
            @pl.when(late)
            def _():
                for way in range(2):
                    more.copy(way, 1, pieces[layer][kind]).start()

            if kind < kinds - 1:

                @pl.when(jnp.logical_not(late))
                def _():
                    for way in range(2):
                        some.copy(way, 1, pieces[layer][kind]).start()

    @pl.when(late)
    def _():
        more.run(short=(kinds - 1,))

    @pl.when(jnp.logical_not(late))
    def _():
        some.run()

    for kind in range(kinds):
        pltpu.make_async_copy(got[kind], got[kind], rs_send.at[kind]).wait()
    pltpu.make_async_copy(others, others, sq_send.at[0]).wait()


def gather_last(n, begun, after, rest, arrived, sent):
    me, at = ring(n)
    late = ends_last()

    @pl.when(jnp.logical_not(late))
    def _():
        pl.delay(PAUSE_NS)

    meet(at)
    layers, rows = begun.shape[0], begun.shape[1] // n
    pieces = [(0, layer, 0, rows, layer * 2 // layers) for layer in range(layers)]
    gather = Gather(n, at, [rest], [rows], [pieces[::step] for step in WAYS], arrived, sent)

    def source(way, steps, layer):
        return begun.at[layer, pl.ds(pl.multiple_of(at(way, -steps) * rows, 16), rows)]

    @pl.when(late)
    def _():
        for way in range(2):
            for piece in gather.order(way, n // 2):
                gather.copy(way, n // 2, piece, source(way, n // 2 - 1, piece[1])).start()
        for way in range(2):
            for piece in gather.order(way, n // 2):
                gather.copy(way, n // 2, piece).wait_recv()
        gather.wait_sent(0, 1)

    @pl.when(jnp.logical_not(late))
    def _():
        for i in range(layers):
            for way in range(2):
                gather.copy(way, 1, gather.orders[way][i], source(way, 0, gather.orders[way][i][1])).start()
        gather.run()


def copy_blocks(n, src, dst, sem, offsets):
    me, at = ring(n)
    rows = src.shape[1] // n
    blocks = [pl.ds(pl.multiple_of(at(0, off) * rows, 16), rows) for off in offsets]
    return [pltpu.make_async_copy(src.at[:, here], dst.at[:, here], sem.at[off]) for here, off in zip(blocks, offsets)]


def run_all(copies):
    for copy in copies:
        copy.start()
    for copy in copies:
        copy.wait()


def write_most(n, *refs):
    *refs, done, sems, block_sems = refs
    whole = [pltpu.make_async_copy(src, dst, sems.at[i]) for i, (src, dst) in enumerate(zip(refs[:9], refs[9:])) if i != 2]
    for copy in whole:
        copy.start()
    done[...] = jnp.zeros_like(done)
    late = ends_last()

    @pl.when(late)
    def _():
        run_all(copy_blocks(n, refs[2], refs[11], block_sems, [off for off in range(n) if off != n // 2]))

    @pl.when(jnp.logical_not(late))
    def _():
        run_all(copy_blocks(n, refs[2], refs[11], block_sems, [0]))

    for copy in whole:
        copy.wait()


def write_rest(n, rest, begun, out, sems):
    late = ends_last()

    @pl.when(late)
    def _():
        run_all(copy_blocks(n, rest, out, sems, [n // 2]))

    @pl.when(jnp.logical_not(late))
    def _():
        run_all(copy_blocks(n, rest, out, sems, range(1, n)))


def solution(mesh):
    n = mesh.shape["dp"]

    def step(*arrays):
        terms, weights, m, v = (arrays[i : i + 3] for i in (0, 3, 6, 9))
        terms = [t[0] for t in terms]
        layers = m[0].shape[0]
        shapes = [one.shape[1:] for one in m]
        count = n * sum(one.size for one in m)
        half = n // 2
        sums = layers // 2 + (half - 1) * layers
        terms_kept = layers // 2 + (half - 2) * layers
        dma = pltpu.SemaphoreType.DMA
        scratch = [pltpu.VMEM((layers, *s), jnp.bfloat16) for s in shapes]
        scratch += [pltpu.VMEM((2, terms_kept, *s), jnp.bfloat16) for s in shapes]
        scratch += [pltpu.VMEM((2, sums, *s), jnp.bfloat16) for s in shapes]
        scratch += [pltpu.VMEM((n, 1, 128), jnp.float32)]
        scratch += [dma((2, 3 * sums)), dma((3,)), dma((3,)), dma((1,)), dma((1,)), dma((3,)), dma((3,)), dma((3, 3))]
        in_vmem, in_hbm = pl.BlockSpec(memory_space=pltpu.VMEM), pl.BlockSpec(memory_space=pltpu.HBM)
        new = [*weights, *m, *v]
        kept = pl.pallas_call(
            functools.partial(sum_and_step, n, layers, count),
            out_shape=[pltpu.VMEM(one.shape, one.dtype) for one in new],
            in_specs=[in_hbm] * 12,
            out_specs=[in_vmem] * 9,
            scratch_shapes=scratch,
            compiler_params=pltpu.CompilerParams(collective_id=0, has_side_effects=True, vmem_limit_bytes=40 * 2**20),
        )(*terms, *weights, *m, *v)
        *written, done = pl.pallas_call(
            functools.partial(write_most, n),
            out_shape=[*(jax.ShapeDtypeStruct(one.shape, one.dtype) for one in new), pltpu.VMEM((8, 128), jnp.float32)],
            in_specs=[in_vmem] * 9,
            out_specs=[in_hbm] * 9 + [in_vmem],
            scratch_shapes=[dma((9,)), dma((n,))],
            compiler_params=pltpu.CompilerParams(vmem_limit_bytes=2**20),
        )(*kept)
        rest = pl.pallas_call(
            functools.partial(gather_last, n),
            out_shape=pltpu.VMEM(weights[2].shape, weights[2].dtype),
            in_specs=[in_vmem, in_vmem],
            out_specs=in_vmem,
            scratch_shapes=[dma((2, half * layers)), dma((1,))],
            compiler_params=pltpu.CompilerParams(collective_id=1, has_side_effects=True, vmem_limit_bytes=2**20),
        )(kept[2], done)
        written[2] = pl.pallas_call(
            functools.partial(write_rest, n),
            out_shape=jax.ShapeDtypeStruct(weights[2].shape, weights[2].dtype),
            in_specs=[in_vmem, in_hbm],
            out_specs=in_hbm,
            input_output_aliases={1: 0},
            scratch_shapes=[dma((n,))],
            compiler_params=pltpu.CompilerParams(vmem_limit_bytes=2**20),
        )(rest, written[2])
        return tuple(written)

    all_of, cut = P(None, None, None), P(None, "dp", None)
    return jax.shard_map(
        step,
        mesh=mesh,
        in_specs=(P(("rep", "dp"), None, None, None),) * 3 + (all_of,) * 3 + (cut,) * 6,
        out_specs=(P("rep", None, None),) * 3 + (P("rep", "dp", None),) * 6,
        check_vma=False,
    )
```
